128 devices in a mesh: seq: 32 (over z_lo, y, x), grp: 4 (over z_hi, core).
Axes of the slice: x: 4, y: 4, z: 4 (z_hi: 2, z_lo: 2; z = z_hi * 2 + z_lo), core: 2. Of those that a mesh axis runs over, the one named last changes fastest.
Arguments:
- queries: bfloat16 [4, 8192, 1536], P('grp', 'seq'), may hold values from -6 to 6
- key_rows: bfloat16 [4, 8192, 1536], P('grp', 'seq'), may hold values from -6 to 6
- value_rows: bfloat16 [4, 8192, 1536], P('grp', 'seq'), may hold values from -6 to 6
- attn_cotangent: bfloat16 [4, 8192, 1536], P('grp', 'seq'), may hold values from -6 to 6
- mixer_input: bfloat16 [4, 4096, 3072], P('grp', 'seq'), may hold values from -6 to 6
- step_raw: bfloat16 [4, 4096, 3072], P('grp', 'seq'), may hold values from -3 to 3
- state_in: bfloat16 [4, 8, 4096], P('grp', None, 'seq'), may hold values from -6 to 6
- state_out: bfloat16 [4, 8, 4096], P('grp', None, 'seq'), may hold values from -6 to 6
- mixer_cotangent: bfloat16 [4, 4096, 3072], P('grp', 'seq'), may hold values from -0.3125 to 0.3125
- decay_log: float32 [8, 3072], replicated, may hold values from -9 to 0.5
- step_bias: float32 [3072], replicated, may hold values from -4 to -1
- skip_gain: float32 [3072], replicated, may hold values from 0.5 to 1.5
Outputs:
- grad_queries: bfloat16 [4, 8192, 1536], P('grp', 'seq')
- grad_keys: bfloat16 [4, 8192, 1536], P('grp', 'seq')
- grad_values: bfloat16 [4, 8192, 1536], P('grp', 'seq')
- grad_input: bfloat16 [4, 4096, 3072], P('grp', 'seq')
- grad_step: bfloat16 [4, 4096, 3072], P('grp', 'seq')
- grad_state_in: bfloat16 [4, 8, 4096], P('grp', None, 'seq')
- grad_state_out: bfloat16 [4, 8, 4096], P('grp', None, 'seq')
- grad_decay_log: float32 [8, 3072], replicated
- grad_step_bias: float32 [3072], replicated
- grad_skip_gain: float32 [3072], replicated
The draws below stay inside these ranges and needn't reach their ends.
All inputs are finite; a program needn't handle non-finite values.
Results may differ from the reference program's by a relative error of at most 0.0097.
Values may be sent and summed in bfloat16 or wider, within the bound.
No kernel may reach another device: no remote copies, remote signals or barrier semaphores. Data moves between devices by JAX's collectives and lax.ppermute only.
A program may use at most 128 MiB of HBM per device.

```python
import jax
import jax.numpy as jnp
from jax import lax

HEADS = 12
HEAD_DIM = 128
INNER = 3072
STATE = 8
WINDOW = 1024
A_TOK = 256
TOKENS = 8192
M_TOKENS = 4096
SEQS = 4


def base_rows(key, salt):
    normal_rows = jax.random.normal(jax.random.fold_in(key, salt), (SEQS, TOKENS, HEADS * HEAD_DIM), jnp.float32)
    return jnp.clip(normal_rows, -6.0, 6.0)


def draw_queries(key, part):
    result = base_rows(key, 11)
    return result.astype(jnp.bfloat16)


def draw_key_rows(key, part):
    result = base_rows(key, 12)
    return result.astype(jnp.bfloat16)


def level_of(key, extent, cuts, least, largest):
    def one(position, shards_of):
        draws = jax.random.uniform(jax.random.fold_in(jax.random.fold_in(key, 6), position), (shards_of,), jnp.float32, least / len(cuts), largest / len(cuts))
        return jnp.repeat(jnp.exp(draws), extent[position] // shards_of).reshape((-1,) + (1,) * (len(extent) - position - 1))

    loudness = one(*cuts[0])
    for cut in cuts[1:]:
        loudness = loudness * one(*cut)
    return loudness


def bell_draw(rng, dims, deviation, most, cuts=(), kind=jnp.bfloat16):
    values = jax.random.normal(rng, dims, jnp.float32) * deviation
    if len(cuts) > 0:
        values = level_of(rng, dims, cuts, -0.22, 0.18) * values
    return jnp.clip(values, min=-most, max=most).astype(kind)


def setup_inputs(seed: int = 0) -> dict:
    key_of = jax.random.split(jax.random.key(seed), 13)
    queries = draw_queries(jax.random.fold_in(key_of[12], 71), 0)
    key_rows = draw_key_rows(jax.random.fold_in(key_of[12], 71), 0)
    value_rows = bell_draw(key_of[2], (SEQS, TOKENS, HEADS * HEAD_DIM), 1.0, 6.0, ((0, 4), (1, 32)))
    attn_cotangent = bell_draw(key_of[3], (SEQS, TOKENS, HEADS * HEAD_DIM), 1.0, 6.0, ((0, 4), (1, 32)))
    mixer_input = bell_draw(key_of[4], (SEQS, M_TOKENS, INNER), 1.0, 6.0, ((0, 4), (1, 32)))
    step_raw = bell_draw(key_of[5], (SEQS, M_TOKENS, INNER), 0.5, 3.0, ((0, 4), (1, 32)))
    state_in = bell_draw(key_of[6], (SEQS, STATE, M_TOKENS), 1.0, 6.0, ((0, 4), (2, 32)))
    state_out = bell_draw(key_of[7], (SEQS, STATE, M_TOKENS), 1.0, 6.0, ((0, 4), (2, 32)))
    mixer_cotangent = bell_draw(key_of[8], (SEQS, M_TOKENS, INNER), 0.05, 0.3125, ((0, 4), (1, 32)))
    decay_log = jnp.clip(jax.random.uniform(key_of[9], (STATE, INNER), jnp.float32, -9.0, 0.5), -9.0, 0.5)
    step_bias = jnp.clip(jax.random.uniform(key_of[10], (INNER,), jnp.float32, -4.0, -1.0), -4.0, -1.0)
    skip_gain = jnp.clip(1.0 + 0.1 * jax.random.normal(key_of[11], (INNER,), jnp.float32), 0.5, 1.5)
    return {"queries": queries, "key_rows": key_rows, "value_rows": value_rows, "attn_cotangent": attn_cotangent, "mixer_input": mixer_input, "step_raw": step_raw, "state_in": state_in, "state_out": state_out, "mixer_cotangent": mixer_cotangent, "decay_log": decay_log, "step_bias": step_bias, "skip_gain": skip_gain}


NEG_BIG = -1e+30

def window_grads(query_block, key_stack, value_stack, grad_block, first_valid):
    block_width = query_block.shape[0]
    stack_rows = key_stack.shape[0]
    lead = stack_rows - block_width
    score_scale = query_block.shape[2] ** (-0.5)
    query_wide = query_block.astype(jnp.float32)
    key_wide = key_stack.astype(jnp.float32)
    value_wide = value_stack.astype(jnp.float32)
    grad_wide = grad_block.astype(jnp.float32)
    scores = jnp.einsum('qhd,khd->hqk', query_wide, key_wide) * score_scale
    row_pos = jnp.arange(block_width)[:, None]
    col_pos = jnp.arange(stack_rows)[None, :]
    allowed = (col_pos <= row_pos + lead) & (col_pos > row_pos + lead - WINDOW) & (col_pos >= first_valid)
    scores = jnp.where(allowed[None], scores, NEG_BIG)
    row_max = lax.optimization_barrier(jnp.max(scores, axis=2, keepdims=True))
    raw_weights = jnp.exp(scores - row_max)
    softmax_prob = raw_weights / lax.optimization_barrier(jnp.sum(raw_weights, axis=2, keepdims=True))
    prob_half = lax.optimization_barrier(softmax_prob.astype(jnp.bfloat16)).astype(jnp.float32)
    output = jnp.einsum('hqk,khd->qhd', prob_half, value_wide)
    row_delta = lax.optimization_barrier(jnp.sum(output * grad_wide, axis=2))
    grad_prob = jnp.einsum('qhd,khd->hqk', grad_wide, value_wide)
    grad_score = softmax_prob * (grad_prob - row_delta.T[:, :, None])
    grad_score = lax.optimization_barrier(grad_score.astype(jnp.bfloat16)).astype(jnp.float32)
    grad_query = jnp.einsum('hqk,khd->qhd', grad_score, key_wide) * score_scale
    grad_key = jnp.einsum('hqk,qhd->khd', grad_score, query_wide) * score_scale
    grad_value = jnp.einsum('hqk,qhd->khd', prob_half, grad_wide)
    return (grad_query, grad_key, grad_value)

def attention_grads(operands):
    queries, key_rows, value_rows, grad_rows = operands
    count = TOKENS // A_TOK
    reach = (WINDOW + A_TOK - 1) // A_TOK
    shape_four = (count, A_TOK, HEADS, HEAD_DIM)
    query_blocks = queries.reshape(shape_four)
    key_blocks = key_rows.reshape(shape_four)
    value_blocks = value_rows.reshape(shape_four)
    grad_blocks = grad_rows.reshape(shape_four)
    pad_shape = (reach, A_TOK, HEADS, HEAD_DIM)
    key_padded = jnp.concatenate([jnp.zeros(pad_shape, key_blocks.dtype), key_blocks], 0)
    value_padded = jnp.concatenate([jnp.zeros(pad_shape, value_blocks.dtype), value_blocks], 0)
    stack_shape = ((reach + 1) * A_TOK, HEADS, HEAD_DIM)

    def one_block(block_index):
        query_block = lax.dynamic_index_in_dim(query_blocks, block_index, 0, keepdims=False)
        grad_block = lax.dynamic_index_in_dim(grad_blocks, block_index, 0, keepdims=False)
        key_stack = lax.dynamic_slice_in_dim(key_padded, block_index, reach + 1, 0).reshape(stack_shape)
        value_stack = lax.dynamic_slice_in_dim(value_padded, block_index, reach + 1, 0).reshape(stack_shape)
        first_valid = jnp.maximum(reach - block_index, 0) * A_TOK
        return window_grads(query_block, key_stack, value_stack, grad_block, first_valid)
    grad_query, grad_key, grad_value = lax.map(one_block, jnp.arange(count, dtype=jnp.int32))
    grad_key = grad_key.reshape(count, reach + 1, A_TOK, HEADS, HEAD_DIM)
    grad_value = grad_value.reshape(count, reach + 1, A_TOK, HEADS, HEAD_DIM)
    total_key = grad_key[:, reach]
    total_value = grad_value[:, reach]
    for distance in range(1, reach + 1):
        padding_rows = jnp.zeros((distance, A_TOK, HEADS, HEAD_DIM), jnp.float32)
        total_key = total_key + jnp.concatenate([grad_key[distance:, reach - distance], padding_rows], 0)
        total_value = total_value + jnp.concatenate([grad_value[distance:, reach - distance], padding_rows], 0)
    width = HEADS * HEAD_DIM
    return (grad_query.reshape(TOKENS, width).astype(jnp.bfloat16), total_key.reshape(TOKENS, width).astype(jnp.bfloat16), total_value.reshape(TOKENS, width).astype(jnp.bfloat16))

def mixer_forward(input_rows, raw_rows, in_proj, out_proj, decay_log, step_bias, skip_gain):
    decay_rate = -jnp.exp(decay_log)
    step_rows = jax.nn.softplus(raw_rows + step_bias)

    def advance(state, item):
        input_now, step_now, in_now, out_now = item
        state = jnp.exp(step_now[None, :] * decay_rate) * state + (step_now * input_now)[None, :] * in_now[:, None]
        return (state, lax.optimization_barrier(jnp.sum(out_now[:, None] * state, axis=0)) + skip_gain * input_now)
    zero_state = jnp.zeros(decay_log.shape, jnp.float32)
    _, output = lax.scan(advance, zero_state, (input_rows, step_rows, in_proj.T, out_proj.T))
    return output

def reference(queries, key_rows, value_rows, attn_cotangent, mixer_input, step_raw, state_in, state_out, mixer_cotangent, decay_log, step_bias, skip_gain):
    grad_queries, grad_keys, grad_values = lax.map(attention_grads, (queries, key_rows, value_rows, attn_cotangent))

    def mixer_grads(pieces):
        input_rows = pieces[0].astype(jnp.float32)
        raw_rows = pieces[1].astype(jnp.float32)
        in_proj = pieces[2].astype(jnp.float32)
        out_proj = pieces[3].astype(jnp.float32)
        cot_rows = pieces[4].astype(jnp.float32)
        _, pullback = jax.vjp(mixer_forward, input_rows, raw_rows, in_proj, out_proj, decay_log, step_bias, skip_gain)
        return pullback(cot_rows)
    grads = lax.map(mixer_grads, (mixer_input, step_raw, state_in, state_out, mixer_cotangent))
    grad_input, grad_step, grad_in, grad_out, grad_decay, grad_bias, grad_skip = grads
    return (grad_queries, grad_keys, grad_values, grad_input.astype(jnp.bfloat16), grad_step.astype(jnp.bfloat16), grad_in.astype(jnp.bfloat16), grad_out.astype(jnp.bfloat16), lax.optimization_barrier(jnp.sum(grad_decay, axis=0)), lax.optimization_barrier(jnp.sum(grad_bias, axis=0)), lax.optimization_barrier(jnp.sum(grad_skip, axis=0)))
```

```python
from functools import partial

import jax
import jax.numpy as jnp
from jax import lax
from jax.experimental import pallas as pl
from jax.experimental.pallas import tpu as pltpu
from jax.sharding import Mesh
from jax.sharding import PartitionSpec as P

HD = 128
SZ, SY, SX, GRP = "seq_0", "seq_1", "seq_2", "grp"
SEQ = (SZ, SY, SX)
BF = jnp.bfloat16
F32 = jnp.float32
NEG = -1e30
VLIM = 60 * 1024 * 1024


def sds(shape, dtype):
    return jax.ShapeDtypeStruct(shape, dtype)


def ring(n, d):
    return [(i, (i + d) % n) for i in range(n)]


def ring_shift(array, axis, d):
    return lax.ppermute(array, axis, ring(lax.axis_size(axis), d))


ANY = pl.BlockSpec(memory_space=pl.ANY)
SMEM = pl.BlockSpec(memory_space=pltpu.SMEM)
VMEM = pl.BlockSpec(memory_space=pltpu.VMEM)


def run_copies(copies):
    for c in copies:
        c.start()
    for c in copies:
        c.wait()


def pack_pair(first, second, me, heads):
    rows = first.shape[0]

    def body(me_ref, a_ref, b_ref, *rest):
        outs, sem = rest[:4], rest[4]
        copies = []
        for d in range(4):
            dest = lax.rem(me_ref[0] + d, 4)
            for c in range(heads):
                col = pl.multiple_of((dest * heads + c) * HD, HD)
                for t, ref in enumerate((a_ref, b_ref)):
                    copies.append(
                        pltpu.make_async_copy(
                            ref.at[:, pl.ds(col, HD)],
                            outs[d].at[c, t],
                            sem.at[d, c, t],
                        )
                    )
        run_copies(copies)

    return pl.pallas_call(
        body,
        out_shape=[sds((heads, 2, rows, HD), BF)] * 4,
        in_specs=[SMEM, ANY, ANY],
        out_specs=[ANY] * 4,
        scratch_shapes=[pltpu.SemaphoreType.DMA((4, heads, 2))],
        name="pack_pair",
    )(me, first, second)


def assemble(pieces, me, heads):
    rows = pieces[0].shape[2]

    def body(me_ref, *rest):
        ins, outs, sem = rest[:4], rest[4 : 4 + heads], rest[4 + heads]
        copies = []
        for d in range(4):
            source = lax.rem(me_ref[0] + 4 - d, 4)
            row = pl.multiple_of(source * rows, rows)
            for c in range(heads):
                copies.append(
                    pltpu.make_async_copy(
                        ins[d].at[c], outs[c].at[:, pl.ds(row, rows)], sem.at[d, c]
                    )
                )
        run_copies(copies)

    return pl.pallas_call(
        body,
        out_shape=[sds((2, 4 * rows, HD), BF)] * heads,
        in_specs=[SMEM] + [ANY] * 4,
        out_specs=[ANY] * heads,
        scratch_shapes=[pltpu.SemaphoreType.DMA((4, heads))],
        name="assemble",
    )(me, *pieces)


def attention_head(qo, kv, kvp, first, blk):
    seg = qo.shape[1]
    nb = seg // blk
    scale = HD ** (-0.5)

    def body(first_ref, qo_ref, kv_ref, kvp_ref, dq_ref, dkv_ref, dkvp_ref, k_s, kt_s, v_s, s_s, p_s, dk_s, dv_s):
        k_s[0:seg] = kvp_ref[0]
        k_s[seg : 2 * seg] = kv_ref[0]
        v_s[0:seg] = kvp_ref[1]
        v_s[seg : 2 * seg] = kv_ref[1]
        for i in range(2 * nb):
            kt_s[i] = k_s[i * blk : (i + 1) * blk].astype(F32).T.astype(BF)
        dk_s[...] = jnp.zeros_like(dk_s)
        dv_s[...] = jnp.zeros_like(dv_s)
        no_prev = jnp.where(first_ref[0] == 1, NEG, 0.0).astype(F32)
        ki = lax.broadcasted_iota(jnp.int32, (blk, blk), 0)
        qi = lax.broadcasted_iota(jnp.int32, (blk, blk), 1)
        nt = (((1,), (1,)), ((), ()))

        def step(b, carry):
            q = qo_ref[0, pl.ds(b * blk, blk)]
            do = qo_ref[1, pl.ds(b * blk, blk)]
            m = jnp.full((1, blk), NEG, F32)
            for kb in range(nb + 1):
                rows = pl.ds((b + kb) * blk, blk)
                s = lax.dot_general(k_s[rows], q, nt, preferred_element_type=F32)
                s = s + jnp.where(b + kb < nb, no_prev, 0.0)
                if kb == 0:
                    s = jnp.where(ki > qi, s, NEG)
                if kb == nb:
                    s = jnp.where(ki <= qi, s, NEG)
                s_s[kb] = s
                m = jnp.maximum(m, jnp.max(s, axis=0, keepdims=True))
            mc = m * scale
            total = jnp.zeros((1, blk), F32)
            dsum = jnp.zeros((1, blk), F32)
            for kb in range(nb + 1):
                rows = pl.ds((b + kb) * blk, blk)
                p = jnp.exp(s_s[kb] * scale - mc)
                dp = lax.dot_general(v_s[rows], do, nt, preferred_element_type=F32)
                s_s[kb] = p
                p_s[kb] = dp
                total = total + jnp.sum(p, axis=0, keepdims=True)
                dsum = dsum + jnp.sum(p * dp, axis=0, keepdims=True)
            inv = 1.0 / total
            delta = dsum * inv
            dqt = jnp.zeros((HD, blk), F32)
            for kb in range(nb + 1):
                rows = pl.ds((b + kb) * blk, blk)
                p = s_s[kb] * inv
                ds = (p * (p_s[kb] - delta)).astype(BF)
                pb = p.astype(BF)
                dv_s[rows] += jnp.dot(pb, do, preferred_element_type=F32)
                dk_s[rows] += jnp.dot(ds, q, preferred_element_type=F32)
                dqt = dqt + jnp.dot(kt_s[b + kb], ds, preferred_element_type=F32)
            dq_ref[pl.ds(b * blk, blk)] = (dqt.T * scale).astype(BF)
            return carry

        lax.fori_loop(0, nb, step, 0)
        dkvp_ref[0] = (dk_s[0:seg] * scale).astype(BF)
        dkvp_ref[1] = dv_s[0:seg].astype(BF)
        dkv_ref[0] = dk_s[seg : 2 * seg] * scale
        dkv_ref[1] = dv_s[seg : 2 * seg]

    return pl.pallas_call(
        body,
        out_shape=[sds((seg, HD), BF), sds((2, seg, HD), F32), sds((2, seg, HD), BF)],
        in_specs=[SMEM, VMEM, VMEM, VMEM],
        out_specs=[VMEM] * 3,
        scratch_shapes=[
            pltpu.VMEM((2 * seg, HD), BF),
            pltpu.VMEM((2 * nb, HD, blk), BF),
            pltpu.VMEM((2 * seg, HD), BF),
            pltpu.VMEM((nb + 1, blk, blk), F32),
            pltpu.VMEM((nb + 1, blk, blk), F32),
            pltpu.VMEM((2 * seg, HD), F32),
            pltpu.VMEM((2 * seg, HD), F32),
        ],
        compiler_params=pltpu.CompilerParams(vmem_limit_bytes=VLIM),
        name="attention_head",
    )(first, qo, kv, kvp)


def add_split(own, back, me, heads, blk):
    def body(me_ref, *rest):
        own_r, back_r, outs = rest[:heads], rest[heads : 2 * heads], rest[2 * heads :]
        for d in range(4):
            row = pl.multiple_of(lax.rem(me_ref[0] + d, 4) * blk, blk)
            for c in range(heads):
                for t in range(2):
                    both = own_r[c][t, pl.ds(row, blk)] + back_r[c][t, pl.ds(row, blk)].astype(F32)
                    outs[d][c, t] = both.astype(BF)

    return pl.pallas_call(
        body,
        out_shape=[sds((heads, 2, blk, HD), BF)] * 4,
        in_specs=[SMEM] + [VMEM] * (2 * heads),
        out_specs=[VMEM] * 4,
        compiler_params=pltpu.CompilerParams(vmem_limit_bytes=VLIM),
        name="add_split",
    )(me, *own, *back)


def split_rows(dqs, me, heads, blk):
    def body(me_ref, *rest):
        ins, outs = rest[:heads], rest[heads:]
        for d in range(4):
            row = pl.multiple_of(lax.rem(me_ref[0] + d, 4) * blk, blk)
            for c in range(heads):
                outs[d][c] = ins[c][pl.ds(row, blk)]

    return pl.pallas_call(
        body,
        out_shape=[sds((heads, blk, HD), BF)] * 4,
        in_specs=[SMEM] + [VMEM] * heads,
        out_specs=[VMEM] * 4,
        name="split_rows",
    )(me, *dqs)


def merge_cols(pieces, me, heads, blk, count):
    def body(me_ref, *rest):
        ins, outs = rest[:4], rest[4 : 4 + count]
        for d in range(4):
            source = lax.rem(me_ref[0] + 4 - d, 4)
            for c in range(heads):
                col = pl.multiple_of((source * heads + c) * HD, HD)
                for t in range(count):
                    outs[t][:, pl.ds(col, HD)] = ins[d][c, t]

    return pl.pallas_call(
        body,
        out_shape=[sds((blk, 4 * heads * HD), BF)] * count,
        in_specs=[SMEM] + [VMEM] * 4,
        out_specs=[VMEM] * count,
        name="merge_cols",
    )(me, *pieces)


def attention_part(queries, key_rows, value_rows, attn_cotangent):
    q, k, v, do = queries[0], key_rows[0], value_rows[0], attn_cotangent[0]
    blk = q.shape[0]
    heads = q.shape[1] // (4 * HD)
    me = lax.axis_index(SX).reshape(1)
    sy, sz = lax.axis_index(SY), lax.axis_index(SZ)
    first = ((sy == 0) & (sz == 0)).astype(jnp.int32).reshape(1)
    ny = lax.axis_size(SY)
    rows = ny * lax.axis_size(SZ)
    kv_out = pack_pair(k, v, me, heads)
    kv_in = [kv_out[0]] + [ring_shift(kv_out[d], SX, d) for d in range(1, 4)]
    qo_out = pack_pair(q, do, me, heads)
    qo_in = [qo_out[0]] + [ring_shift(qo_out[d], SX, d) for d in range(1, 4)]
    kv_seg = assemble(kv_in, me, heads)
    down = [(i, i + 1) for i in range(rows - 1)]
    up = [(i + 1, i) for i in range(rows - 1)]
    kv_prev = [lax.ppermute(kv_seg[c], (SZ, SY), down) for c in range(heads)]
    qo_seg = assemble(qo_in, me, heads)
    dqs, own, back = [], [], []
    for c in range(heads):
        dq, dkv, dkvp = attention_head(qo_seg[c], kv_seg[c], kv_prev[c], first, blk)
        dqs.append(dq)
        own.append(dkv)
        back.append(lax.ppermute(dkvp, (SZ, SY), up))
    dq_out = split_rows(dqs, me, heads, blk)
    dq_in = [dq_out[0]] + [ring_shift(dq_out[d], SX, d) for d in range(1, 4)]
    dkv_out = add_split(own, back, me, heads, blk)
    dkv_in = [dkv_out[0]] + [ring_shift(dkv_out[d], SX, d) for d in range(1, 4)]
    (grad_q,) = merge_cols([p[:, None] for p in dq_in], me, heads, blk, 1)
    grad_k, grad_v = merge_cols(dkv_in, me, heads, blk, 2)
    return grad_q[None], grad_k[None], grad_v[None]


TILE = 1024
SUB = TILE // HD


def rows_of(t):
    return pl.ds((t // 8) * (8 * SUB) + t % 8, SUB, stride=8)


def mixer_prologue(x_ref, raw_ref, cot_ref, bias_ref, dt_s, dtx_s, cot_s, tokens, x_s=None):
    def load(i, carry):
        for c in range(SUB):
            cols = slice(c * HD, (c + 1) * HD)
            raw = raw_ref[pl.ds(i * 16, 16), cols].astype(F32) + bias_ref[:, cols]
            x = x_ref[pl.ds(i * 16, 16), cols].astype(F32)
            cot = cot_ref[pl.ds(i * 16, 16), cols].astype(F32)
            dt = jnp.maximum(raw, 0.0) + jnp.log(1.0 + jnp.exp(-jnp.abs(raw)))
            dtx = dt * x
            for half in range(2):
                dst = pl.ds(i * (16 * SUB) + half * (8 * SUB) + c * 8, 8)
                part = slice(half * 8, half * 8 + 8)
                dt_s[dst] = dt[part]
                dtx_s[dst] = dtx[part]
                cot_s[dst] = cot[part]
        return carry

    lax.fori_loop(0, tokens // 16, load, 0)


def load_rates(decay_ref, a_s, nstate):
    for c in range(SUB):
        a_s[c * nstate : (c + 1) * nstate] = -jnp.exp(decay_ref[:, c * HD : (c + 1) * HD])


def splat(ref, row):
    return ref[pl.ds(row, SUB, stride=0), :]


def mixer_totals(x, raw, cot, decay_log, bias, b_rows, c_rows):
    tokens, inner = x.shape
    nstate = decay_log.shape[0]
    steps = inner // TILE

    def body(x_ref, raw_ref, cot_ref, decay_ref, bias_ref, b_ref, c_ref, pay_ref, dt_s, dtx_s, cot_s, a_s):
        mixer_prologue(x_ref, raw_ref, cot_ref, bias_ref, dt_s, dtx_s, cot_s, tokens)
        load_rates(decay_ref, a_s, nstate)
        rate = [a_s[pl.ds(n, SUB, stride=nstate), :] for n in range(nstate)]

        def group(i, carry):
            h, prod, back, total = carry
            h, prod, back = list(h), list(prod), list(back)
            for s in range(8):
                idx = pl.ds(i * (8 * SUB) + s, SUB, stride=8)
                dt, dtx, ct = dt_s[idx, :], dtx_s[idx, :], cot_s[idx, :]
                total = total + dt
                for n in range(nstate):
                    row = (i * 8 + s) * nstate + n
                    a = jnp.exp(dt * rate[n])
                    h[n] = a * h[n] + dtx * splat(b_ref, row)
                    prod[n] = prod[n] * a
                    back[n] = back[n] + prod[n] * (ct * splat(c_ref, row))
            return tuple(h), tuple(prod), tuple(back), total

        zero = jnp.zeros((SUB, HD), F32)
        one = jnp.ones((SUB, HD), F32)
        h, _, back, total = lax.fori_loop(
            0,
            tokens // 8,
            group,
            ((zero,) * nstate, (one,) * nstate, (zero,) * nstate, zero),
        )
        hi = total.astype(BF).astype(F32)
        for n in range(nstate):
            pay_ref[n] = h[n].astype(BF)
            pay_ref[nstate + n] = back[n].astype(BF)
        pay_ref[2 * nstate] = total.astype(BF)
        pay_ref[2 * nstate + 1] = (total - hi).astype(BF)

    tok_spec = pl.BlockSpec((tokens, TILE), lambda j: (0, j))
    full = pl.BlockSpec((tokens * nstate, HD), lambda j: (0, 0))
    return pl.pallas_call(
        body,
        grid=(steps,),
        out_shape=sds((steps, 2 * nstate + 2, SUB, HD), BF),
        in_specs=[
            tok_spec,
            tok_spec,
            tok_spec,
            pl.BlockSpec((nstate, TILE), lambda j: (0, j)),
            pl.BlockSpec((1, TILE), lambda j: (0, j)),
            full,
            full,
        ],
        out_specs=pl.BlockSpec((None, 2 * nstate + 2, SUB, HD), lambda j: (j, 0, 0, 0)),
        scratch_shapes=[pltpu.VMEM((tokens * SUB, HD), F32)] * 3
        + [pltpu.VMEM((nstate * SUB, HD), F32)],
        compiler_params=pltpu.CompilerParams(vmem_limit_bytes=VLIM),
        name="mixer_totals",
    )(x, raw, cot, decay_log, bias, b_rows, c_rows)


def combine_ring(pieces, me, decay_log, size):
    steps, width, _, _ = pieces[0].shape
    nstate = decay_log.shape[0]

    def body(me_ref, decay_ref, *rest):
        ins = rest[:size]
        pay_ref, pre_ref, suf_ref, tb_ref, ta_ref, buf, a_s = rest[size:]
        mine = me_ref[0]
        for d in range(size):
            buf[lax.rem(mine + size - d, size)] = ins[d][...]
        for j in range(steps):
            for c in range(SUB):
                lo = j * TILE + c * HD
                a_s[c * nstate : (c + 1) * nstate] = -jnp.exp(decay_ref[:, lo : lo + HD])
            totals = [
                buf[k, j, 2 * nstate].astype(F32) + buf[k, j, 2 * nstate + 1].astype(F32)
                for k in range(size)
            ]
            zero = jnp.zeros((SUB, HD), F32)
            before = after = zero
            for k in range(size):
                before = before + jnp.where(k < mine, totals[k], zero)
                after = after + jnp.where(k > mine, totals[k], zero)
            whole = sum(totals[1:], totals[0])
            tb_ref[j] = before
            ta_ref[j] = after
            pay_ref[j, 2 * nstate] = whole.astype(BF)
            pay_ref[j, 2 * nstate + 1] = (whole - whole.astype(BF).astype(F32)).astype(BF)
            for n in range(nstate):
                rate = a_s[pl.ds(n, SUB, stride=nstate), :]
                decay = [jnp.exp(rate * totals[k]) for k in range(size)]
                run, pre = zero, zero
                for k in range(size):
                    pre = jnp.where(k == mine, run, pre)
                    run = decay[k] * run + buf[k, j, n].astype(F32)
                pay_ref[j, n] = run.astype(BF)
                pre_ref[j, n] = pre
                run, suf = zero, zero
                for k in reversed(range(size)):
                    suf = jnp.where(k == mine, run, suf)
                    run = decay[k] * run + buf[k, j, nstate + n].astype(F32)
                pay_ref[j, nstate + n] = run.astype(BF)
                suf_ref[j, n] = suf

    carry = sds((steps, nstate, SUB, HD), F32)
    chan = sds((steps, SUB, HD), F32)
    return pl.pallas_call(
        body,
        out_shape=[sds(pieces[0].shape, BF), carry, carry, chan, chan],
        in_specs=[SMEM] + [VMEM] * (1 + size),
        out_specs=[VMEM] * 5,
        scratch_shapes=[
            pltpu.VMEM((size,) + pieces[0].shape, BF),
            pltpu.VMEM((nstate * SUB, HD), F32),
        ],
        compiler_params=pltpu.CompilerParams(vmem_limit_bytes=VLIM),
        name="combine_ring",
    )(me, decay_log, *pieces)


def mixer_backward(x, raw, cot, decay_log, bias, gain, b_rows, c_rows, levels):
    tokens, inner = x.shape
    nstate = decay_log.shape[0]
    steps = inner // TILE
    depth = len(levels)

    def body(*refs):
        x_ref, raw_ref, cot_ref, decay_ref, bias_ref, gain_ref, b_ref, c_ref = refs[:8]
        lev = [refs[8 + 4 * i : 12 + 4 * i] for i in range(depth)]
        rest = refs[8 + 4 * depth :]
        gx_ref, graw_ref, db_ref, dc_ref, rate_ref, gbias_ref, gskip_ref = rest[:7]
        dt_s, dtx_s, cot_s, a_s, dec_s, h_s, prod_s, proj_s, ddt_s, b_acc, c_acc = rest[7:]
        j = pl.program_id(0)
        mixer_prologue(x_ref, raw_ref, cot_ref, bias_ref, dt_s, dtx_s, cot_s, tokens)
        load_rates(decay_ref, a_s, nstate)
        rate = [a_s[pl.ds(n, SUB, stride=nstate), :] for n in range(nstate)]
        start, finish = [], []
        for n in range(nstate):
            pre = lev[depth - 1][0][n]
            suf = lev[depth - 1][1][n]
            for i in reversed(range(depth - 1)):
                pre = lev[i][0][n] + jnp.exp(rate[n] * lev[i][2][...]) * pre
                suf = lev[i][1][n] + jnp.exp(rate[n] * lev[i][3][...]) * suf
            start.append(pre)
            finish.append(suf)
            h_s[pl.ds(n * SUB, SUB), :] = pre

        def forward(i, h):
            h = list(h)
            for s in range(8):
                idx = pl.ds(i * (8 * SUB) + s, SUB, stride=8)
                dt, dtx, ct = dt_s[idx, :], dtx_s[idx, :], cot_s[idx, :]
                for n in range(nstate):
                    row = (i * 8 + s) * nstate + n
                    a = jnp.exp(dt * rate[n])
                    h[n] = a * h[n] + dtx * splat(b_ref, row)
                    at = pl.ds(pl.multiple_of(row * SUB, SUB), SUB)
                    dec_s[at, :] = a
                    h_s[pl.ds(pl.multiple_of((row + nstate) * SUB, SUB), SUB), :] = h[n]
                    prod_s[at, :] = h[n] * ct
            return tuple(h)

        lax.fori_loop(0, tokens // 8, forward, tuple(start))

        def fold(acc):
            def one(i, carry):
                base = i * (8 * SUB)
                parts = [prod_s[pl.ds(base + c, 8, stride=SUB), :] for c in range(SUB)]
                while len(parts) > 1:
                    parts = [parts[k] + parts[k + 1] for k in range(0, len(parts), 2)]
                at = pl.ds(pl.multiple_of(i * 8, 8), 8)
                old = jnp.where(j == 0, jnp.zeros_like(parts[0]), acc[at, :])
                acc[at, :] = old + parts[0]
                return carry

            lax.fori_loop(0, tokens * nstate // 8, one, 0, unroll=8)

        fold(c_acc)

        def backward(k, carry):
            i = tokens // 8 - 1 - k
            ag, acc = list(carry[0]), list(carry[1])
            for s in reversed(range(8)):
                idx = pl.ds(i * (8 * SUB) + s, SUB, stride=8)
                dt, dtx, ct = dt_s[idx, :], dtx_s[idx, :], cot_s[idx, :]
                proj, ddt = [], []
                for n in range(nstate):
                    row = (i * 8 + s) * nstate + n
                    at = pl.ds(pl.multiple_of(row * SUB, SUB), SUB)
                    g = ct * splat(c_ref, row) + ag[n]
                    proj.append(g * splat(b_ref, row))
                    prod_s[at, :] = g * dtx
                    ag[n] = g * dec_s[at, :]
                    w = ag[n] * h_s[at, :]
                    acc[n] = acc[n] + w * dt
                    ddt.append(w * rate[n])
                while len(proj) > 1:
                    proj = [proj[m] + proj[m + 1] for m in range(0, len(proj), 2)]
                    ddt = [ddt[m] + ddt[m + 1] for m in range(0, len(ddt), 2)]
                proj_s[idx, :] = proj[0]
                ddt_s[idx, :] = ddt[0]
            return tuple(ag), tuple(acc)

        zero = jnp.zeros((SUB, HD), F32)
        _, acc = lax.fori_loop(0, tokens // 8, backward, (tuple(finish), (zero,) * nstate))
        for n in range(nstate):
            rate_ref[n] = acc[n] * rate[n]
        fold(b_acc)

        def epilogue(i, carry):
            sums_b, sums_s = list(carry[0]), list(carry[1])
            for c in range(SUB):
                cols = slice(c * HD, (c + 1) * HD)
                x16 = x_ref[pl.ds(i * 16, 16), cols].astype(F32)
                cot16 = cot_ref[pl.ds(i * 16, 16), cols].astype(F32)
                src = [pl.ds(i * (16 * SUB) + half * (8 * SUB) + c * 8, 8) for half in range(2)]
                proj = jnp.concatenate([proj_s[at, :] for at in src], 0)
                ddt = jnp.concatenate([ddt_s[at, :] for at in src], 0)
                dt = jnp.concatenate([dt_s[at, :] for at in src], 0)
                gx_ref[pl.ds(i * 16, 16), cols] = (gain_ref[:, cols] * cot16 + dt * proj).astype(BF)
                graw = (x16 * proj + ddt) * (1.0 - jnp.exp(-dt))
                graw_ref[pl.ds(i * 16, 16), cols] = graw.astype(BF)
                skip = cot16 * x16
                sums_b[c] = sums_b[c] + graw[0:8] + graw[8:16]
                sums_s[c] = sums_s[c] + skip[0:8] + skip[8:16]
            return tuple(sums_b), tuple(sums_s)

        zero8 = jnp.zeros((8, HD), F32)
        sums_b, sums_s = lax.fori_loop(
            0, tokens // 16, epilogue, ((zero8,) * SUB, (zero8,) * SUB)
        )
        for c in range(SUB):
            gbias_ref[c : c + 1, :] = jnp.sum(sums_b[c], axis=0, keepdims=True)
            gskip_ref[c : c + 1, :] = jnp.sum(sums_s[c], axis=0, keepdims=True)

        @pl.when(j == steps - 1)
        def _():
            nt = (((1,), (1,)), ((), ()))
            ones = jnp.ones((8, HD), BF)
            for acc_ref, out in ((b_acc, db_ref), (c_acc, dc_ref)):
                full = acc_ref[...]
                hi = full.astype(BF)
                lo = (full - hi.astype(F32)).astype(BF)
                out[...] = lax.dot_general(
                    ones, hi, nt, preferred_element_type=F32
                ) + lax.dot_general(ones, lo, nt, preferred_element_type=F32)

    tok_spec = pl.BlockSpec((tokens, TILE), lambda j: (0, j))
    row_spec = pl.BlockSpec((1, TILE), lambda j: (0, j))
    full = pl.BlockSpec((tokens * nstate, HD), lambda j: (0, 0))
    state_spec = pl.BlockSpec((None, nstate, SUB, HD), lambda j: (j, 0, 0, 0))
    chan_spec = pl.BlockSpec((None, SUB, HD), lambda j: (j, 0, 0))
    sum_spec = pl.BlockSpec((8, tokens * nstate), lambda j: (0, 0))
    level_args = [part for level in levels for part in level]
    return pl.pallas_call(
        body,
        grid=(steps,),
        out_shape=[
            sds((tokens, inner), BF),
            sds((tokens, inner), BF),
            sds((8, tokens * nstate), F32),
            sds((8, tokens * nstate), F32),
            sds((steps, nstate, SUB, HD), F32),
            sds((steps, SUB, HD), F32),
            sds((steps, SUB, HD), F32),
        ],
        in_specs=[
            tok_spec,
            tok_spec,
            tok_spec,
            pl.BlockSpec((nstate, TILE), lambda j: (0, j)),
            row_spec,
            row_spec,
            full,
            full,
        ]
        + [state_spec, state_spec, chan_spec, chan_spec] * depth,
        out_specs=[tok_spec, tok_spec, sum_spec, sum_spec, state_spec, chan_spec, chan_spec],
        scratch_shapes=[pltpu.VMEM((tokens * SUB, HD), F32)] * 3
        + [pltpu.VMEM((nstate * SUB, HD), F32)]
        + [
            pltpu.VMEM((tokens * nstate * SUB, HD), F32),
            pltpu.VMEM(((tokens + 1) * nstate * SUB, HD), F32),
            pltpu.VMEM((tokens * nstate * SUB, HD), F32),
        ]
        + [pltpu.VMEM((tokens * SUB, HD), F32)] * 2
        + [pltpu.VMEM((tokens * nstate, HD), F32)] * 2,
        compiler_params=pltpu.CompilerParams(vmem_limit_bytes=VLIM),
        name="mixer_backward",
    )(x, raw, cot, decay_log, bias, gain, b_rows, c_rows, *level_args)


def pair_sum(array, axis, distance):
    size = lax.axis_size(axis)
    return array + lax.ppermute(array, axis, [(i, i ^ distance) for i in range(size)])


def mixer_part(
    mixer_input, step_raw, state_in, state_out, mixer_cotangent, decay_log, step_bias, skip_gain
):
    x, raw, cot = mixer_input[0], step_raw[0], mixer_cotangent[0]
    tokens, inner = x.shape
    nstate = decay_log.shape[0]
    bias, gain = step_bias.reshape(1, inner), skip_gain.reshape(1, inner)

    def lanes(proj):
        return jnp.broadcast_to(proj[0].astype(F32).T.reshape(tokens * nstate, 1), (tokens * nstate, HD))

    b_rows, c_rows = lanes(state_in), lanes(state_out)
    payload = mixer_totals(x, raw, cot, decay_log, bias, b_rows, c_rows)
    levels = []
    for axis in reversed(SEQ):
        size = lax.axis_size(axis)
        pieces = [payload] + [ring_shift(payload, axis, d) for d in range(1, size)]
        payload, *level = combine_ring(pieces, lax.axis_index(axis).reshape(1), decay_log, size)
        levels.append(level)
    grad_x, grad_raw, db, dc, rate, gbias, gskip = mixer_backward(
        x, raw, cot, decay_log, bias, gain, b_rows, c_rows, levels
    )
    steps = inner // TILE
    summed = jnp.concatenate([rate, gbias[:, None], gskip[:, None]], 1)
    for axis in (SX, SY, SZ, GRP):
        distance = 1
        while distance < lax.axis_size(axis):
            summed = pair_sum(summed, axis, distance)
            distance *= 2
    grad_decay = jnp.moveaxis(summed[:, :nstate], 1, 0).reshape(nstate, inner)

    def rows(sums):
        return sums[0].reshape(tokens, nstate).T.astype(BF)[None]

    return (
        grad_x[None],
        grad_raw[None],
        rows(db),
        rows(dc),
        grad_decay,
        summed[:, nstate].reshape(inner),
        summed[:, nstate + 1].reshape(inner),
    )


def on_device(
    queries,
    key_rows,
    value_rows,
    attn_cotangent,
    mixer_input,
    step_raw,
    state_in,
    state_out,
    mixer_cotangent,
    decay_log,
    step_bias,
    skip_gain,
):
    attention = attention_part(queries, key_rows, value_rows, attn_cotangent)
    mixer = mixer_part(
        mixer_input, step_raw, state_in, state_out, mixer_cotangent, decay_log, step_bias, skip_gain
    )
    return attention + mixer


def solution(mesh):
    torus = Mesh(mesh.devices.reshape(2, 4, 4, mesh.shape[GRP]), SEQ + (GRP,))
    tok = P(GRP, SEQ, None)
    lane = P(GRP, None, SEQ)
    in_specs = (tok, tok, tok, tok, tok, tok, lane, lane, tok, P(), P(), P())
    out_specs = (tok, tok, tok, tok, tok, lane, lane, P(), P(), P())
    return jax.shard_map(
        on_device, mesh=torus, in_specs=in_specs, out_specs=out_specs, check_vma=False
    )
```
